32 devices in a mesh: lon: 16 (over z, y, core), band: 2 (over x).
Axes of the slice: x: 2, y: 2, z: 4, core: 2. Of those that a mesh axis runs over, the one named last changes fastest.
Arguments:
- nest_field: float32 [32, 96, 9216], P(None, 'band', 'lon'), may hold values from -6 to 6
- nest_area: float32 [96, 9216], P('band', 'lon'), may hold values from 0.5 to 2
- parent_field: float32 [32, 32, 3072], P(None, 'band', 'lon'), may hold values from -6 to 6
- nest_offset: int32 [1], replicated, may hold values from 576 to 9215
- relax_rate: float32 [32], replicated, may hold values from 0.3 to 0.8
- zonal_coef: float32 [32], replicated, may hold values from 0.05 to 0.24
- merid_coef: float32 [32], replicated, may hold values from 0.05 to 0.24
Outputs:
- parent_out: float32 [32, 32, 3072], P(None, 'band', 'lon')
The draws below stay inside these ranges and needn't reach their ends.
All inputs are finite; a program needn't handle non-finite values.
Results may differ from the reference program's by a relative error of at most 0.000084.
Values sent between devices are 32-bit elements; how exact they have to be, the bound alone decides.
A program may use at most 64 MiB of HBM per device.

```python
import math
import jax
import jax.numpy as jnp

NXP = 3072
LV = 32
NS = 3
NYP = 32
NYN = 96
NXN = 9216
N_LON = 16


def block_levels(stream_key, shape, split, low, largest):
    def one(axis_at, blocks):
        draws = jax.random.uniform(jax.random.fold_in(jax.random.fold_in(stream_key, 6), axis_at), (blocks,), jnp.float32, low / len(split), largest / len(split))
        return jnp.repeat(jnp.exp(draws), shape[axis_at] // blocks).reshape((-1,) + (1,) * (len(shape) - axis_at - 1))

    level = one(*split[0])
    for cut in split[1:]:
        level = level * one(*cut)
    return level


def centred(key, shape, scale, bound, cuts=(), kind=jnp.bfloat16):
    factor_of = block_levels(key, shape, cuts, -0.22, 0.18) if cuts else 1.0
    result = jax.random.normal(key, shape, jnp.float32) * scale * factor_of
    return jnp.minimum(jnp.maximum(result, -bound), bound).astype(kind)


def setup_inputs(seed: int = 0) -> dict:
    streams_of = jax.random.split(jax.random.key(seed), 8)
    return {
        "nest_field": centred(streams_of[0], (LV, NYN, NXN), 1.0, 6.0, ((1, 2), (2, 16)), jnp.float32),
        "nest_area": jnp.clip(jnp.exp(math.log(2.0) - 1.3862944 * jax.random.uniform(streams_of[1], (NYN, NXN), jnp.float32) ** block_levels(streams_of[1], (NYN, NXN), ((0, 2), (1, 16)), -0.2, 0.2)), 0.5, 2.0),
        "parent_field": centred(streams_of[2], (LV, NYP, NXP), 1.0, 6.0, ((1, 2), (2, 16)), jnp.float32),
        "nest_offset": jax.random.randint(streams_of[3], (1,), 3 * NXP // N_LON, 3 * NXP).astype(jnp.int32),
        "relax_rate": jnp.clip(jax.random.uniform(streams_of[4], (LV,), jnp.float32, 0.3, 0.8), 0.3, 0.8),
        "zonal_coef": jnp.clip(jax.random.uniform(streams_of[5], (LV,), jnp.float32, 0.05, 0.24), 0.05, 0.24),
        "merid_coef": jnp.clip(jax.random.uniform(streams_of[6], (LV,), jnp.float32, 0.05, 0.24), 0.05, 0.24),
    }


def zonal_pass(field, coef):
    left = jnp.roll(field, 1, axis=2)
    right = jnp.roll(field, -1, axis=2)
    return field + coef[:, None, None] * (left - 2.0 * field + right)


def merid_pass(field, coef):
    padded = jnp.pad(field, ((0, 0), (1, 1), (0, 0)))
    return field + coef[:, None, None] * (padded[:, :-2] - 2.0 * field + padded[:, 2:])


def reference(nest_field, nest_area, parent_field, nest_offset, relax_rate, zonal_coef, merid_coef):
    offset_cells = nest_offset[0]
    stacked = jnp.concatenate([nest_field * nest_area[None], nest_area[None]], axis=0)
    planes = stacked.shape[0]
    row_sums = stacked.reshape(planes, NYP, 3, NXN).sum(axis=2)
    rolled = jnp.roll(row_sums, offset_cells, axis=2)
    cell_sums = rolled.reshape(planes, NYP, NXP, 3).sum(axis=3)
    restricted = cell_sums[:LV] / cell_sums[LV][None]
    field = parent_field + relax_rate[:, None, None] * (restricted - parent_field)
    for sweep in range(NS):
        field = zonal_pass(field, zonal_coef)
        field = merid_pass(field, merid_coef)
    return field
```

```python
import functools

import jax
import jax.numpy as jnp
from jax import lax
from jax.experimental import pallas as pl
from jax.experimental.pallas import tpu as pltpu
from jax.sharding import PartitionSpec as P

NS = 3
HALO = NS
LANES = 128
HALF = LANES // 2
GROUP = 8
SMOOTH = 4
BLEND_LAG, SMOOTH_LAG = 2, 3
MESH = pl.DeviceIdType.MESH
BULK, EAST, WEST, UP, DOWN, EDGES = range(6)


def chunk_width(par_cols):
    return max(w for w in range(1, HALF + 1) if par_cols % w == 0)


def rolled(x, by):
    by %= LANES
    return pltpu.roll(x, by, 1) if by else x


def kernel(
    shift, forward, width, off_ref, nest_hbm, area_hbm, parent_hbm, relax_hbm, zonal_hbm, merid_hbm,
    out_ref, nest, area, parent, relax, zonal, merid, select, spill, packed, got, east_out, east_got,
    west_out, west_got, edge_out, edge_got, share, field, up_out, up_got, down_out, down_got,
    in_sems, send_sems, recv_sems,
):
    lon, band = lax.axis_index("lon"), lax.axis_index("band")
    lons, bands = lax.axis_size("lon"), lax.axis_size("band")
    levels, rows, cols = parent.shape
    lanes = field.shape[2]
    count = cols // width
    tail = lanes - cols
    blocks = levels // GROUP
    split = (count + 1) // 2
    gone = list(range(split)) if forward else list(range(split, count))
    bulk = shift % lons != 0
    has_above, has_below = band > 0, band < bands - 1

    def at(ahead):
        return lax.rem(lon + ahead % lons, lons)

    barrier = pltpu.get_barrier_semaphore()

    def greet(x, y):
        pl.semaphore_signal(barrier, inc=1, device_id=(x, y), device_id_type=MESH)

    partners = [1, -1] + ([shift, -shift] if bulk else [])
    for ahead in partners:
        greet(at(ahead), band)

    @pl.when(has_above)
    def _():
        greet(lon, band - 1)

    @pl.when(has_below)
    def _():
        greet(lon, band + 1)

    def load(index, source, target):
        return pltpu.make_async_copy(source, target, in_sems.at[index])

    def nest_load(block):
        part = pl.ds(block * GROUP, GROUP)
        return load(block, nest_hbm.at[part], nest.at[part])

    area_load = load(blocks, area_hbm, area)
    parent_load = load(blocks + 1, parent_hbm, parent)
    small = [
        load(blocks + 2 + k, source, target)
        for k, (source, target) in enumerate(
            [(relax_hbm, relax), (zonal_hbm, zonal), (merid_hbm, merid)]
        )
    ]
    area_load.start()
    for b in range(blocks):
        nest_load(b).start()
    parent_load.start()
    for one in small:
        one.start()

    def copy(kind, index, source, target, x, y):
        return pltpu.make_async_remote_copy(
            src_ref=source,
            dst_ref=target,
            send_sem=send_sems.at[kind],
            recv_sem=recv_sems.at[kind * (blocks + 1) + index],
            device_id=(x, y),
            device_id_type=MESH,
        )

    def bulk_copy(index, first, size):
        part = pl.ds(first, size)
        return copy(BULK, index, packed.at[part], got.at[part], at(shift), band)

    def east_copy(index, first, size):
        part = pl.ds(first, size)
        return copy(EAST, index, east_out.at[part], east_got.at[part], at(1), band)

    def west_copy(index, first, size):
        part = pl.ds(first, size)
        return copy(WEST, index, west_out.at[part], west_got.at[part], at(-1), band)

    def edge_copy(index):
        return copy(
            EDGES, index, edge_out.at[index], edge_got.at[index], at(1 if index else -1), band
        )

    def up_copy(index):
        return copy(UP, index, up_out.at[index], up_got.at[index], lon, band - 1)

    def down_copy(index):
        return copy(DOWN, index, down_out.at[index], down_got.at[index], lon, band + 1)

    arrived = got if bulk else packed
    offset = off_ref[0]
    start = lax.rem(lax.div(offset, 3), cols)
    within = lax.rem(start, width)
    lane = lax.broadcasted_iota(jnp.int32, (8, LANES), 1)
    low = lane < HALF
    spot = jnp.where(low, lane, lane - HALF)
    before = {c: spot < start - c * width for c in gone}
    here = {c: spot == start - c * width for c in gone}
    zero = jnp.zeros((8, LANES), jnp.float32)
    place = spot // 4
    is_right = spot < HALO
    is_left = (spot >= tail - HALO) & (spot < tail)

    def pack(values):
        tiles = []
        if width == HALF:
            for p in range(values.shape[1] // LANES):
                top = values[:8, p * LANES : (p + 1) * LANES]
                bottom = values[8:, p * LANES : (p + 1) * LANES]
                tiles.append(jnp.where(low, top, rolled(bottom, HALF)))
                tiles.append(jnp.where(low, rolled(top, HALF), bottom))
            return tiles
        pad = jnp.zeros((8, HALF - width), jnp.float32)
        for k in range(count + 1):
            part = values[:, k * width : (k + 1) * width]
            tiles.append(jnp.concatenate([part[:8], pad, part[8:], pad], axis=1))
        return tiles

    def unpack(tiles, end):
        if width == HALF and tail == HALF and count % 2:
            tiles = tiles + [end]
            top, bottom = [], []
            for x, y in zip(tiles[::2], tiles[1::2]):
                top.append(jnp.where(low, x, rolled(y, HALF)))
                bottom.append(jnp.where(low, rolled(x, HALF), y))
        else:
            top = [t[:, :width] for t in tiles] + [end[:, :tail]]
            bottom = [t[:, HALF : HALF + width] for t in tiles] + [end[:, HALF : HALF + tail]]
        return jnp.concatenate(
            [jnp.concatenate(top, axis=1), jnp.concatenate(bottom, axis=1)], axis=0
        )

    def first_part(tile, edge, k):
        rest = rolled(edge, -k)
        return {c: jnp.where(before[c], tile(c), jnp.where(here[c], rest, 0.0)) for c in gone}

    def second_part(tile):
        return {c: jnp.where(before[c], 0.0, tile(c)) for c in gone}

    def sent(tile, edge, k):
        return first_part(tile, edge, k) if forward else second_part(tile)

    def kept(tile, edge, k):
        parts = {c: tile(c) for c in range(count)}
        parts.update(second_part(tile) if forward else first_part(tile, edge, k))
        return parts

    def sums(values, planes, first):
        high = values.astype(jnp.bfloat16)
        rest = (values - high.astype(jnp.float32)).astype(jnp.bfloat16)
        by_column = jnp.dot(high, select[...], preferred_element_type=jnp.float32) + jnp.dot(
            rest, select[...], preferred_element_type=jnp.float32
        )
        edge = zero
        for k in range(planes):
            tiles = pack(by_column[k * rows : (k + 1) * rows])
            for c in range(count):
                packed[first + k * count + c] = tiles[c]
            edge = edge + rolled(tiles[count], k)
        packed[first + planes * count] = edge

    unit = GROUP * count + 1
    last = blocks * unit

    spread = select.shape[1]
    slot_of = lax.broadcasted_iota(jnp.int32, (8, spread), 1)
    column = jnp.where(slot_of >= start, slot_of - start, slot_of - start + cols)
    column = jnp.where(
        slot_of < cols, column, jnp.where(slot_of == cols + within, cols, -HALF)
    )
    lowest = (column * 3 - lax.rem(offset, 3))[:1]
    strip = max(n for n in range(16, 65, 16) if select.shape[0] % n == 0)
    ramp = lax.broadcasted_iota(jnp.int32, (strip, spread), 0) - lowest

    def choose(step, carry):
        cell = ramp + step * strip
        hit = (cell >= 0) & (cell < 3)
        select[pl.ds(pl.multiple_of(step * strip, strip), strip), :] = jnp.where(
            hit, 1.0, 0.0
        ).astype(jnp.bfloat16)
        return carry

    lax.fori_loop(0, select.shape[0] // strip, choose, 0)

    cells = area.shape[1]

    def by_rows(planes):
        height = planes[0].shape[0]
        for t in range(spill.shape[0]):
            edge = min(cells, (t + 1) * LANES)
            for k, plane in enumerate(planes):
                spill[t, k * height : (k + 1) * height, : edge - t * LANES] = plane[:, t * LANES : edge]
        third = len(planes) * rows
        tiles = []
        for t in range(spill.shape[0]):
            edge = min(cells, (t + 1) * LANES)
            tile = (
                spill.at[t][pl.ds(0, third, stride=3), :]
                + spill.at[t][pl.ds(1, third, stride=3), :]
                + spill.at[t][pl.ds(2, third, stride=3), :]
            )
            tiles.append(tile[:, : edge - t * LANES])
        return jnp.concatenate(tiles, axis=1)

    area_load.wait()
    sums(by_rows([area[...]]), 1, last)
    pl.semaphore_wait(
        barrier, len(partners) + has_above.astype(jnp.int32) + has_below.astype(jnp.int32)
    )
    if bulk:
        bulk_copy(blocks, last, count + 1).start()

    def front(block, carry):
        nest_load(block).wait()
        weight = area[...]
        planes = [nest[block * GROUP + k] * weight for k in range(GROUP)]
        sums(by_rows(planes), GROUP, block * unit)
        if bulk:
            bulk_copy(block, block * unit, unit).start()
        return carry

    lax.fori_loop(0, blocks, front, 0)

    parent_load.wait()
    blank = jnp.zeros((rows, tail), jnp.float32)
    head = (cols - HALO) // LANES * LANES

    def edges(block, carry):
        first, final = zero, zero
        for k in range(GROUP):
            wide = jnp.concatenate([parent[block * GROUP + k], blank], axis=1)
            for half, part in enumerate([wide[:8], wide[8:]]):
                mine = (place == k) & (low if half == 0 else ~low)
                to = 4 * k + HALF * half
                first = jnp.where(mine, rolled(part[:, :LANES], to), first)
                end = part[:, head : head + LANES]
                final = jnp.where(mine, rolled(end, to - (cols - HALO - head)), final)
        edge_out[0, block] = first
        edge_out[1, block] = final
        return carry

    lax.fori_loop(0, blocks, edges, 0)
    for side in range(2):
        edge_copy(side).start()

    @pl.when(jnp.logical_not(has_above))
    def _():
        down_got[...] = jnp.zeros_like(down_got)

    @pl.when(jnp.logical_not(has_below))
    def _():
        up_got[...] = jnp.zeros_like(up_got)

    def tile_of(first):
        return lambda c: arrived[first + c]

    main = len(gone)

    def sizes(planes):
        return (planes * main + 1, 1) if forward else (1, planes * main + 1)

    def hand_on(first, planes, index, target):
        edge = arrived[first + planes * count]
        east_pack, west_pack = zero, zero
        for k in range(planes):
            tile = tile_of(first + k * count)
            out = sent(tile, edge, k)
            keep = kept(tile, edge, k)
            main_out = east_out if forward else west_out
            for j, c in enumerate(gone):
                main_out[target[0 if forward else 1] + k * main + j] = out[c]
            mine = place == k
            east_pack = jnp.where(
                mine, rolled(keep[count - 1], 4 * k - (width - HALO)), east_pack
            )
            west_pack = jnp.where(mine, rolled(keep[0], 4 * k), west_pack)
        east_size, west_size = sizes(planes)
        east_out[target[0] + east_size - 1] = east_pack
        west_out[target[1] + west_size - 1] = west_pack
        east_copy(index, target[0], east_size).start()
        west_copy(index, target[1], west_size).start()

    def assembled(first, planes, k, target, fill):
        edge = arrived[first + planes * count]
        tile = tile_of(first + k * count)
        out = sent(tile, edge, k)
        parts = kept(tile, edge, k)
        east_size, west_size = sizes(planes)
        main_got = east_got if forward else west_got
        for j, c in enumerate(gone):
            value = main_got[target[0 if forward else 1] + k * main + j]
            parts[c] = parts[c] + value
        left = rolled(east_got[target[0] + east_size - 1], tail - HALO - 4 * k)
        right = rolled(west_got[target[1] + west_size - 1], -4 * k)
        if forward:
            right = right + out[0]
        else:
            left = left + rolled(out[count - 1], tail - width)
        end = jnp.where(is_right, right, jnp.where(is_left, left, fill))
        return unpack([parts[c] for c in range(count)], end)

    def targets(block):
        east_size, west_size = sizes(GROUP)
        return block * east_size, block * west_size

    def wait_sides(index, planes, target):
        east_size, west_size = sizes(planes)
        east_copy(index, target[0], east_size).wait_recv()
        west_copy(index, target[1], west_size).wait_recv()

    if bulk:
        bulk_copy(blocks, last, count + 1).wait_recv()
    hand_on(last, 1, blocks, targets(blocks))

    def take(block):
        if bulk:
            bulk_copy(block, block * unit, unit).wait_recv()
        hand_on(block * unit, GROUP, block, targets(block))

    def blend(block):
        @pl.when(block == 0)
        def _():
            wait_sides(blocks, 1, targets(blocks))
            share[...] = 1.0 / assembled(last, 1, 0, targets(blocks), 1.0)
            for one in small:
                one.wait()
            for side in range(2):
                edge_copy(side).wait_recv()

        wait_sides(block, GROUP, targets(block))
        from_east, from_west = edge_got[0, block], edge_got[1, block]
        for k in range(GROUP):
            level = block * GROUP + k
            ratio = assembled(block * unit, GROUP, k, targets(block), 0.0) * share[...]
            end = jnp.where(
                is_right,
                rolled(from_east, -4 * k),
                jnp.where(is_left, rolled(from_west, tail - HALO - 4 * k), 0.0),
            )
            ends = jnp.concatenate([end[:, :tail], end[:, HALF : HALF + tail]], axis=0)
            before_it = jnp.concatenate([parent[level], ends], axis=1)
            value = before_it + relax[level] * (ratio - before_it)
            field[level] = value
            for j in range(HALO):
                up_out[block, j, k : k + 1, :] = value[j : j + 1]
                down_out[block, j, k : k + 1, :] = value[rows - HALO + j : rows - HALO + j + 1]

        @pl.when(has_above)
        def _():
            up_copy(block).start()

        @pl.when(has_below)
        def _():
            down_copy(block).start()

    tall = rows + 8
    row = lax.broadcasted_iota(jnp.int32, (tall, lanes), 0)
    valid = (
        (row < rows)
        | ((row < rows + HALO) & has_below)
        | ((row >= tall - HALO) & has_above)
    )
    spare = jnp.zeros((8 - 2 * HALO, lanes), jnp.float32)

    def smooth(block):
        @pl.when(has_above)
        def _():
            down_copy(block).wait_recv()

        @pl.when(has_below)
        def _():
            up_copy(block).wait_recv()

        def some(step, carry):
            group = [step * SMOOTH + g for g in range(SMOOTH)]
            values = []
            for k in group:
                extra = [up_got[block, j, pl.ds(k, 1), :] for j in range(HALO)] + [spare]
                extra += [down_got[block, j, pl.ds(k, 1), :] for j in range(HALO)]
                values.append(jnp.concatenate([field[block * GROUP + k]] + extra, axis=0))
            zonals = [zonal[block * GROUP + k] for k in group]
            merids = [merid[block * GROUP + k] for k in group]
            for sweep in range(NS):
                sides = [pltpu.roll(v, 1, 1) + pltpu.roll(v, lanes - 1, 1) for v in values]
                values = [v + z * (s - 2.0 * v) for v, z, s in zip(values, zonals, sides)]
                sides = [pltpu.roll(v, 1, 0) + pltpu.roll(v, tall - 1, 0) for v in values]
                values = [
                    jnp.where(valid, v + m * (s - 2.0 * v), 0.0)
                    for v, m, s in zip(values, merids, sides)
                ]
            for k, value in zip(group, values):
                out_ref[block * GROUP + k] = value[:rows, :cols]
            return carry

        lax.fori_loop(0, GROUP // SMOOTH, some, 0)

    def turn(step, carry):
        @pl.when(step < blocks)
        def _():
            take(step)

        @pl.when((step >= BLEND_LAG) & (step < blocks + BLEND_LAG))
        def _():
            blend(step - BLEND_LAG)

        @pl.when(step >= SMOOTH_LAG)
        def _():
            smooth(step - SMOOTH_LAG)

        return carry

    lax.fori_loop(0, blocks + SMOOTH_LAG, turn, 0)

    def sent_all(kind, source, target):
        copy(kind, 0, source, target, lon, band).wait_send()

    if bulk:
        sent_all(BULK, packed, got)
    sent_all(EAST, east_out, east_got)
    sent_all(WEST, west_out, west_got)
    sent_all(EDGES, edge_out, edge_got)

    @pl.when(has_above)
    def _():
        sent_all(UP, up_out, up_got)

    @pl.when(has_below)
    def _():
        sent_all(DOWN, down_out, down_got)


def fused(shift, forward, width, number, offset, nest, area, parent, relax, zonal, merid):
    levels, rows, cols = parent.shape
    cells = nest.shape[2]
    count = cols // width
    lanes = (cols + 2 * HALO + LANES - 1) // LANES * LANES
    spread = ((count + 1) * width + LANES - 1) // LANES * LANES
    blocks = levels // GROUP
    assert count > 1 and rows == 16 and levels % GROUP == 0 and 4 * GROUP <= HALF
    main = (count + 1) // 2 if forward else count // 2
    many, few = blocks * (GROUP * main + 1) + main + 1, blocks + 1
    east_tiles, west_tiles = (many, few) if forward else (few, many)
    moved = blocks * (GROUP * count + 1) + count + 1

    def tiles(*shape):
        return pltpu.VMEM(shape + (8, LANES), jnp.float32)

    strip = pltpu.VMEM((blocks, HALO, GROUP, lanes), jnp.float32)
    hbm = pl.BlockSpec(memory_space=pl.ANY)
    scalars = pltpu.SMEM((levels,), jnp.float32)
    return pl.pallas_call(
        functools.partial(kernel, shift, forward, width),
        out_shape=jax.ShapeDtypeStruct(parent.shape, jnp.float32),
        in_specs=[pl.BlockSpec(memory_space=pltpu.SMEM)] + [hbm] * 6,
        out_specs=pl.BlockSpec(memory_space=pltpu.VMEM),
        scratch_shapes=[
            pltpu.VMEM(nest.shape, jnp.float32),
            pltpu.VMEM(area.shape, jnp.float32),
            pltpu.VMEM(parent.shape, jnp.float32),
            scalars,
            scalars,
            scalars,
            pltpu.VMEM((cells, spread), jnp.bfloat16),
            pltpu.VMEM(((cells + LANES - 1) // LANES, GROUP * nest.shape[1], LANES), jnp.float32),
            tiles(moved),
            tiles(moved),
            tiles(east_tiles),
            tiles(east_tiles),
            tiles(west_tiles),
            tiles(west_tiles),
            tiles(2, blocks),
            tiles(2, blocks),
            pltpu.VMEM((rows, lanes), jnp.float32),
            pltpu.VMEM((levels, rows, lanes), jnp.float32),
            strip,
            strip,
            strip,
            strip,
            pltpu.SemaphoreType.DMA((blocks + 5,)),
            pltpu.SemaphoreType.DMA((6,)),
            pltpu.SemaphoreType.DMA((5 * (blocks + 1) + 2,)),
        ],
        compiler_params=pltpu.CompilerParams(
            collective_id=number, has_side_effects=True, vmem_limit_bytes=24 << 20
        ),
    )(offset, nest, area, parent, relax, zonal, merid)


def on_device(nest_field, nest_area, parent_field, nest_offset, relax_rate, zonal_coef, merid_coef):
    cols = parent_field.shape[2]
    width = chunk_width(cols)
    count = cols // width
    branches = []
    for steps in range(1, lax.axis_size("lon")):
        for forward in (True, False):
            shift = steps if forward else steps + 1
            branches.append(functools.partial(fused, shift, forward, width, len(branches)))
    place = lax.div(nest_offset[0], 3 * width)
    late = lax.rem(place, count) >= (count + 1) // 2
    return lax.switch(
        2 * (lax.div(place, count) - 1) + late.astype(jnp.int32),
        branches,
        nest_offset,
        nest_field,
        nest_area,
        parent_field,
        relax_rate,
        zonal_coef,
        merid_coef,
    )


def solution(mesh):
    placed = (P(None, "band", "lon"), P("band", "lon"), P(None, "band", "lon"), P(), P(), P(), P())
    return jax.shard_map(
        on_device, mesh=mesh, in_specs=placed, out_specs=P(None, "band", "lon"), check_vma=False
    )
```

```python
import functools

import jax
import jax.numpy as jnp
from jax import lax
from jax.experimental import pallas as pl
from jax.experimental.pallas import tpu as pltpu
from jax.sharding import PartitionSpec as P

NS = 3
HALO = NS
LANES = 128
HALF = LANES // 2
GROUP = 8
SMOOTH = 4
ORDER = ((0, 0), (1, 3), (2, 6))
MESH = pl.DeviceIdType.MESH
BULK, EAST, WEST, UP, DOWN, EDGES, DETOUR, ONWARD = range(8)


def routed(loads, here, there, amount):
    y, z = here
    while z != there[1]:
        step = 1 if there[1] > z else -1
        loads[y, z, step, 0] = loads.get((y, z, step, 0), 0) + amount
        z += step
    if y != there[0]:
        loads[y, z, 0, 1] = loads.get((y, z, 0, 1), 0) + amount


def detour(shift, forward, blocks, spots, part):
    total = len(spots)
    if not total or shift % total == 0:
        return 0, (), 0
    best = None
    for turn, choices in ((-2, ((), (3,), (2,), (2, 3))), (2, ((0,), (1,), (0, 1)))):
        for chosen in choices:
            for number in range(1, blocks) if chosen else (0,):
                loads = {}
                for here in range(total):
                    there = (here + shift) % total
                    share = number / blocks if here % 4 in chosen else 0
                    by = (here + turn) % total
                    if share and (spots[there][0] != spots[by][0] or there == by):
                        break
                    routed(loads, spots[here], spots[by], share)
                    routed(loads, spots[by], spots[there], share)
                    routed(loads, spots[here], spots[there], 1 - share)
                    beside = (here + (1 if forward else -1)) % total
                    routed(loads, spots[here], spots[beside], part)
                else:
                    key = (max(loads.values()) + (0.2 if number else 0.0), number)
                    if best is None or key < best[0]:
                        best = key, (turn, chosen, number)
    return best[1]


def chunk_width(par_cols):
    return max(w for w in range(1, HALF + 1) if par_cols % w == 0)


def rolled(x, by):
    by %= LANES
    return pltpu.roll(x, by, 1) if by else x


def kernel(
    shift, forward, width, way, off_ref, nest_hbm, area_hbm, parent_hbm, relax_hbm, zonal_hbm, merid_hbm,
    out_ref, nest, area, parent, relax, zonal, merid, select, spill, packed, got, east_out, east_got,
    west_out, west_got, edge_out, edge_got, hop, share, field, up_out, up_got, down_out, down_got,
    in_sems, send_sems, recv_sems,
):
    lon, band = lax.axis_index("lon"), lax.axis_index("band")
    lons, bands = lax.axis_size("lon"), lax.axis_size("band")
    levels, rows, cols = parent.shape
    lanes = field.shape[2]
    count = cols // width
    tail = lanes - cols
    blocks = levels // GROUP
    split = (count + 1) // 2
    gone = list(range(split)) if forward else list(range(split, count))
    bulk = shift % lons != 0
    has_above, has_below = band > 0, band < bands - 1

    def at(ahead):
        return lax.rem(lon + ahead % lons, lons)

    barrier = pltpu.get_barrier_semaphore()

    def greet(x, y):
        pl.semaphore_signal(barrier, inc=1, device_id=(x, y), device_id_type=MESH)

    turn, chosen, detours = way
    partners = [1, -1] + ([shift, -shift] if bulk else [])
    if detours:
        partners += [turn, -turn, shift - turn, turn - shift]

        def among(index):
            found = lax.rem(index, 4) == chosen[0]
            for one in chosen[1:]:
                found = found | (lax.rem(index, 4) == one)
            return found

        leaves, helps = among(lon), among(at(-turn))
    for ahead in partners:
        greet(at(ahead), band)

    @pl.when(has_above)
    def _():
        greet(lon, band - 1)

    @pl.when(has_below)
    def _():
        greet(lon, band + 1)

    def load(index, source, target):
        return pltpu.make_async_copy(source, target, in_sems.at[index])

    def nest_load(block):
        part = pl.ds(block * GROUP, GROUP)
        return load(block, nest_hbm.at[part], nest.at[part])

    area_load = load(blocks, area_hbm, area)
    parent_load = load(blocks + 1, parent_hbm, parent)
    small = [
        load(blocks + 2 + k, source, target)
        for k, (source, target) in enumerate(
            [(relax_hbm, relax), (zonal_hbm, zonal), (merid_hbm, merid)]
        )
    ]
    area_load.start()
    for b in range(blocks):
        nest_load(b).start()
    parent_load.start()
    for one in small:
        one.start()

    unit = GROUP * count + 1
    last = blocks * unit
    kinds = [BULK, EAST, WEST, UP, DOWN, EDGES, DETOUR]
    lengths = [blocks + 1, blocks + 1, blocks + 1, blocks, blocks, 2, detours]
    firsts = {kind: sum(lengths[:i]) for i, kind in enumerate(kinds)}

    def copy(kind, index, source, target, x, y, at_target=None):
        first = firsts[kind if at_target is None else at_target]
        return pltpu.make_async_remote_copy(
            src_ref=source,
            dst_ref=target,
            send_sem=send_sems.at[kind],
            recv_sem=recv_sems.at[first + index],
            device_id=(x, y),
            device_id_type=MESH,
        )

    def bulk_copy(index, first, size):
        part = pl.ds(first, size)
        return copy(BULK, index, packed.at[part], got.at[part], at(shift), band)

    def detour_copy(index):
        part = pl.ds(index * unit, unit)
        return copy(DETOUR, index, packed.at[part], hop.at[part], at(turn), band)

    def onward_copy(index):
        part = pl.ds(index * unit, unit)
        return copy(
            ONWARD, index, hop.at[part], got.at[part], at(shift - turn), band, BULK
        )

    def east_copy(index, first, size):
        part = pl.ds(first, size)
        return copy(EAST, index, east_out.at[part], east_got.at[part], at(1), band)

    def west_copy(index, first, size):
        part = pl.ds(first, size)
        return copy(WEST, index, west_out.at[part], west_got.at[part], at(-1), band)

    def edge_copy(index):
        return copy(
            EDGES, index, edge_out.at[index], edge_got.at[index], at(1 if index else -1), band
        )

    def up_copy(index):
        return copy(UP, index, up_out.at[index], up_got.at[index], lon, band - 1)

    def down_copy(index):
        return copy(DOWN, index, down_out.at[index], down_got.at[index], lon, band + 1)

    arrived = got if bulk else packed
    offset = off_ref[0]
    start = lax.rem(lax.div(offset, 3), cols)
    within = lax.rem(start, width)
    lane = lax.broadcasted_iota(jnp.int32, (8, LANES), 1)
    low = lane < HALF
    spot = jnp.where(low, lane, lane - HALF)
    before = {c: spot < start - c * width for c in gone}
    here = {c: spot == start - c * width for c in gone}
    zero = jnp.zeros((8, LANES), jnp.float32)
    place = spot // 4
    is_right = spot < HALO
    is_left = (spot >= tail - HALO) & (spot < tail)

    def pack(values):
        tiles = []
        if width == HALF:
            for p in range(values.shape[1] // LANES):
                top = values[:8, p * LANES : (p + 1) * LANES]
                bottom = values[8:, p * LANES : (p + 1) * LANES]
                tiles.append(jnp.where(low, top, rolled(bottom, HALF)))
                tiles.append(jnp.where(low, rolled(top, HALF), bottom))
            return tiles
        pad = jnp.zeros((8, HALF - width), jnp.float32)
        for k in range(count + 1):
            part = values[:, k * width : (k + 1) * width]
            tiles.append(jnp.concatenate([part[:8], pad, part[8:], pad], axis=1))
        return tiles

    def unpack(tiles, end):
        if width == HALF and tail == HALF and count % 2:
            tiles = tiles + [end]
            top, bottom = [], []
            for x, y in zip(tiles[::2], tiles[1::2]):
                top.append(jnp.where(low, x, rolled(y, HALF)))
                bottom.append(jnp.where(low, rolled(x, HALF), y))
        else:
            top = [t[:, :width] for t in tiles] + [end[:, :tail]]
            bottom = [t[:, HALF : HALF + width] for t in tiles] + [end[:, HALF : HALF + tail]]
        return jnp.concatenate(
            [jnp.concatenate(top, axis=1), jnp.concatenate(bottom, axis=1)], axis=0
        )

    def first_part(tile, edge, k):
        rest = rolled(edge, -k)
        return {c: jnp.where(before[c], tile(c), jnp.where(here[c], rest, 0.0)) for c in gone}

    def second_part(tile):
        return {c: jnp.where(before[c], 0.0, tile(c)) for c in gone}

    def sent(tile, edge, k):
        return first_part(tile, edge, k) if forward else second_part(tile)

    def kept(tile, edge, k):
        parts = {c: tile(c) for c in range(count)}
        parts.update(second_part(tile) if forward else first_part(tile, edge, k))
        return parts

    def sums(values, planes, first):
        high = values.astype(jnp.bfloat16)
        rest = (values - high.astype(jnp.float32)).astype(jnp.bfloat16)
        by_column = jnp.dot(high, select[...], preferred_element_type=jnp.float32) + jnp.dot(
            rest, select[...], preferred_element_type=jnp.float32
        )
        edge = zero
        for k in range(planes):
            tiles = pack(by_column[k * rows : (k + 1) * rows])
            for c in range(count):
                packed[first + k * count + c] = tiles[c]
            edge = edge + rolled(tiles[count], k)
        packed[first + planes * count] = edge

    spread = select.shape[1]
    slot_of = lax.broadcasted_iota(jnp.int32, (8, spread), 1)
    column = jnp.where(slot_of >= start, slot_of - start, slot_of - start + cols)
    column = jnp.where(
        slot_of < cols, column, jnp.where(slot_of == cols + within, cols, -HALF)
    )
    lowest = (column * 3 - lax.rem(offset, 3))[:1]
    strip = max(n for n in range(16, 65, 16) if select.shape[0] % n == 0)
    ramp = lax.broadcasted_iota(jnp.int32, (strip, spread), 0) - lowest

    def choose(step, carry):
        cell = ramp + step * strip
        hit = (cell >= 0) & (cell < 3)
        select[pl.ds(pl.multiple_of(step * strip, strip), strip), :] = jnp.where(
            hit, 1.0, 0.0
        ).astype(jnp.bfloat16)
        return carry

    lax.fori_loop(0, select.shape[0] // strip, choose, 0)

    cells = area.shape[1]

    def by_rows(planes):
        height = planes[0].shape[0]
        for t in range(spill.shape[0]):
            edge = min(cells, (t + 1) * LANES)
            for k, plane in enumerate(planes):
                spill[t, k * height : (k + 1) * height, : edge - t * LANES] = plane[:, t * LANES : edge]
        third = len(planes) * rows
        tiles = []
        for t in range(spill.shape[0]):
            edge = min(cells, (t + 1) * LANES)
            tile = (
                spill.at[t][pl.ds(0, third, stride=3), :]
                + spill.at[t][pl.ds(1, third, stride=3), :]
                + spill.at[t][pl.ds(2, third, stride=3), :]
            )
            tiles.append(tile[:, : edge - t * LANES])
        return jnp.concatenate(tiles, axis=1)

    area_load.wait()
    sums(by_rows([area[...]]), 1, last)
    pl.semaphore_wait(
        barrier, len(partners) + has_above.astype(jnp.int32) + has_below.astype(jnp.int32)
    )
    if bulk:
        bulk_copy(blocks, last, count + 1).start()

    def front(block, carry):
        nest_load(block).wait()
        weight = area[...]
        planes = [nest[block * GROUP + k] * weight for k in range(GROUP)]
        sums(by_rows(planes), GROUP, block * unit)
        if detours:
            around = leaves & (block < detours)

            @pl.when(around)
            def _():
                detour_copy(block).start()

            @pl.when(jnp.logical_not(around))
            def _():
                bulk_copy(block, block * unit, unit).start()
        elif bulk:
            bulk_copy(block, block * unit, unit).start()
        return carry

    lax.fori_loop(0, blocks, front, 0)

    parent_load.wait()
    blank = jnp.zeros((rows, tail), jnp.float32)
    head = (cols - HALO) // LANES * LANES

    def edges(block, carry):
        first, final = zero, zero
        for k in range(GROUP):
            wide = jnp.concatenate([parent[block * GROUP + k], blank], axis=1)
            for half, part in enumerate([wide[:8], wide[8:]]):
                mine = (place == k) & (low if half == 0 else ~low)
                to = 4 * k + HALF * half
                first = jnp.where(mine, rolled(part[:, :LANES], to), first)
                end = part[:, head : head + LANES]
                final = jnp.where(mine, rolled(end, to - (cols - HALO - head)), final)
        edge_out[0, block] = first
        edge_out[1, block] = final
        return carry

    lax.fori_loop(0, blocks, edges, 0)
    for side in range(2):
        edge_copy(side).start()

    @pl.when(jnp.logical_not(has_above))
    def _():
        down_got[...] = jnp.zeros_like(down_got)

    @pl.when(jnp.logical_not(has_below))
    def _():
        up_got[...] = jnp.zeros_like(up_got)

    def tile_of(first):
        return lambda c: arrived[first + c]

    main = len(gone)

    def sizes(planes):
        return (planes * main + 1, 1) if forward else (1, planes * main + 1)

    def hand_on(first, planes, index, target):
        edge = arrived[first + planes * count]
        east_pack, west_pack = zero, zero
        for k in range(planes):
            tile = tile_of(first + k * count)
            out = sent(tile, edge, k)
            keep = kept(tile, edge, k)
            main_out = east_out if forward else west_out
            for j, c in enumerate(gone):
                main_out[target[0 if forward else 1] + k * main + j] = out[c]
            mine = place == k
            east_pack = jnp.where(
                mine, rolled(keep[count - 1], 4 * k - (width - HALO)), east_pack
            )
            west_pack = jnp.where(mine, rolled(keep[0], 4 * k), west_pack)
        east_size, west_size = sizes(planes)
        east_out[target[0] + east_size - 1] = east_pack
        west_out[target[1] + west_size - 1] = west_pack
        east_copy(index, target[0], east_size).start()
        west_copy(index, target[1], west_size).start()

    def assembled(first, planes, k, target, fill):
        edge = arrived[first + planes * count]
        tile = tile_of(first + k * count)
        out = sent(tile, edge, k)
        parts = kept(tile, edge, k)
        east_size, west_size = sizes(planes)
        main_got = east_got if forward else west_got
        for j, c in enumerate(gone):
            value = main_got[target[0 if forward else 1] + k * main + j]
            parts[c] = parts[c] + value
        left = rolled(east_got[target[0] + east_size - 1], tail - HALO - 4 * k)
        right = rolled(west_got[target[1] + west_size - 1], -4 * k)
        if forward:
            right = right + out[0]
        else:
            left = left + rolled(out[count - 1], tail - width)
        end = jnp.where(is_right, right, jnp.where(is_left, left, fill))
        return unpack([parts[c] for c in range(count)], end)

    def targets(block):
        east_size, west_size = sizes(GROUP)
        return block * east_size, block * west_size

    def wait_sides(index, planes, target):
        east_size, west_size = sizes(planes)
        east_copy(index, target[0], east_size).wait_recv()
        west_copy(index, target[1], west_size).wait_recv()

    if bulk:
        bulk_copy(blocks, last, count + 1).wait_recv()
    hand_on(last, 1, blocks, targets(blocks))

    def place_of(due):
        return lax.rem(due + detours, blocks) if detours else due

    def take(due):
        block = place_of(due)
        if detours:

            @pl.when(helps & (due < detours))
            def _():
                detour_copy(due).wait_recv()
                onward_copy(due).start()

        if bulk:
            bulk_copy(block, block * unit, unit).wait_recv()
        hand_on(block * unit, GROUP, block, targets(block))

    def blend(due):
        block = place_of(due)

        @pl.when(due == 0)
        def _():
            wait_sides(blocks, 1, targets(blocks))
            share[...] = 1.0 / assembled(last, 1, 0, targets(blocks), 1.0)
            for one in small:
                one.wait()
            for side in range(2):
                edge_copy(side).wait_recv()

        wait_sides(block, GROUP, targets(block))
        from_east, from_west = edge_got[0, block], edge_got[1, block]
        for k in range(GROUP):
            level = block * GROUP + k
            ratio = assembled(block * unit, GROUP, k, targets(block), 0.0) * share[...]
            end = jnp.where(
                is_right,
                rolled(from_east, -4 * k),
                jnp.where(is_left, rolled(from_west, tail - HALO - 4 * k), 0.0),
            )
            ends = jnp.concatenate([end[:, :tail], end[:, HALF : HALF + tail]], axis=0)
            before_it = jnp.concatenate([parent[level], ends], axis=1)
            value = before_it + relax[level] * (ratio - before_it)
            field[level] = value
            for j in range(HALO):
                up_out[block, j, k : k + 1, :] = value[j : j + 1]
                down_out[block, j, k : k + 1, :] = value[rows - HALO + j : rows - HALO + j + 1]

        @pl.when(has_above)
        def _():
            up_copy(block).start()

        @pl.when(has_below)
        def _():
            down_copy(block).start()

    tall = rows + 8
    row = lax.broadcasted_iota(jnp.int32, (tall, lanes), 0)
    valid = (
        (row < rows)
        | ((row < rows + HALO) & has_below)
        | ((row >= tall - HALO) & has_above)
    )
    spare = jnp.zeros((8 - 2 * HALO, lanes), jnp.float32)

    def smooth(due):
        block = place_of(due)

        @pl.when(has_above)
        def _():
            down_copy(block).wait_recv()

        @pl.when(has_below)
        def _():
            up_copy(block).wait_recv()

        def some(step, carry):
            group = [step * SMOOTH + g for g in range(SMOOTH)]
            values = []
            for k in group:
                extra = [up_got[block, j, pl.ds(k, 1), :] for j in range(HALO)] + [spare]
                extra += [down_got[block, j, pl.ds(k, 1), :] for j in range(HALO)]
                values.append(jnp.concatenate([field[block * GROUP + k]] + extra, axis=0))
            zonals = [zonal[block * GROUP + k] for k in group]
            merids = [merid[block * GROUP + k] for k in group]
            for sweep in range(NS):
                sides = [pltpu.roll(v, 1, 1) + pltpu.roll(v, lanes - 1, 1) for v in values]
                values = [v + z * (s - 2.0 * v) for v, z, s in zip(values, zonals, sides)]
                sides = [pltpu.roll(v, 1, 0) + pltpu.roll(v, tall - 1, 0) for v in values]
                values = [
                    jnp.where(valid, v + m * (s - 2.0 * v), 0.0)
                    for v, m, s in zip(values, merids, sides)
                ]
            for k, value in zip(group, values):
                out_ref[block * GROUP + k] = value[:rows, :cols]
            return carry

        lax.fori_loop(0, GROUP // SMOOTH, some, 0)

    def advance(step, carry):
        for stage, lag in ORDER:
            due = step - lag

            @pl.when((due >= 0) & (due < blocks))
            def _():
                [take, blend, smooth][stage](due)

        return carry

    lax.fori_loop(0, blocks + max(lag for _, lag in ORDER), advance, 0)

    def sent_all(kind, source, target):
        copy(kind, 0, source, target, lon, band).wait_send()

    if detours:
        early = pl.ds(0, detours * unit)
        later = pl.ds(detours * unit, packed.shape[0] - detours * unit)

        @pl.when(leaves)
        def _():
            sent_all(DETOUR, packed.at[early], hop)
            sent_all(BULK, packed.at[later], got.at[later])

        @pl.when(jnp.logical_not(leaves))
        def _():
            sent_all(BULK, packed, got)

        @pl.when(helps)
        def _():
            copy(ONWARD, 0, hop, got.at[early], lon, band, BULK).wait_send()
    elif bulk:
        sent_all(BULK, packed, got)
    sent_all(EAST, east_out, east_got)
    sent_all(WEST, west_out, west_got)
    sent_all(EDGES, edge_out, edge_got)

    @pl.when(has_above)
    def _():
        sent_all(UP, up_out, up_got)

    @pl.when(has_below)
    def _():
        sent_all(DOWN, down_out, down_got)


def fused(shift, forward, width, spots, number, offset, nest, area, parent, relax, zonal, merid):
    levels, rows, cols = parent.shape
    cells = nest.shape[2]
    count = cols // width
    lanes = (cols + 2 * HALO + LANES - 1) // LANES * LANES
    spread = ((count + 1) * width + LANES - 1) // LANES * LANES
    blocks = levels // GROUP
    assert count > 1 and rows == 16 and levels % GROUP == 0 and 4 * GROUP <= HALF
    main = (count + 1) // 2 if forward else count // 2
    way = detour(shift, forward, blocks, spots, main / count)
    unit = GROUP * count + 1
    many, few = blocks * (GROUP * main + 1) + main + 1, blocks + 1
    east_tiles, west_tiles = (many, few) if forward else (few, many)
    moved = blocks * (GROUP * count + 1) + count + 1

    def tiles(*shape):
        return pltpu.VMEM(shape + (8, LANES), jnp.float32)

    strip = pltpu.VMEM((blocks, HALO, GROUP, lanes), jnp.float32)
    hbm = pl.BlockSpec(memory_space=pl.ANY)
    scalars = pltpu.SMEM((levels,), jnp.float32)
    return pl.pallas_call(
        functools.partial(kernel, shift, forward, width, way),
        out_shape=jax.ShapeDtypeStruct(parent.shape, jnp.float32),
        in_specs=[pl.BlockSpec(memory_space=pltpu.SMEM)] + [hbm] * 6,
        out_specs=pl.BlockSpec(memory_space=pltpu.VMEM),
        scratch_shapes=[
            pltpu.VMEM(nest.shape, jnp.float32),
            pltpu.VMEM(area.shape, jnp.float32),
            pltpu.VMEM(parent.shape, jnp.float32),
            scalars,
            scalars,
            scalars,
            pltpu.VMEM((cells, spread), jnp.bfloat16),
            pltpu.VMEM(((cells + LANES - 1) // LANES, GROUP * nest.shape[1], LANES), jnp.float32),
            tiles(moved),
            tiles(moved),
            tiles(east_tiles),
            tiles(east_tiles),
            tiles(west_tiles),
            tiles(west_tiles),
            tiles(2, blocks),
            tiles(2, blocks),
            tiles(max(way[2], 1) * unit),
            pltpu.VMEM((rows, lanes), jnp.float32),
            pltpu.VMEM((levels, rows, lanes), jnp.float32),
            strip,
            strip,
            strip,
            strip,
            pltpu.SemaphoreType.DMA((blocks + 5,)),
            pltpu.SemaphoreType.DMA((8 if way[2] else 6,)),
            pltpu.SemaphoreType.DMA((5 * blocks + 5 + way[2],)),
        ],
        compiler_params=pltpu.CompilerParams(
            collective_id=number, has_side_effects=True, vmem_limit_bytes=24 << 20
        ),
    )(offset, nest, area, parent, relax, zonal, merid)


def on_device(spots, nest_field, nest_area, parent_field, nest_offset, relax_rate, zonal_coef, merid_coef):
    cols = parent_field.shape[2]
    width = chunk_width(cols)
    count = cols // width
    branches = []
    for steps in range(1, lax.axis_size("lon")):
        for forward in (True, False):
            shift = steps if forward else steps + 1
            branches.append(functools.partial(fused, shift, forward, width, spots, len(branches)))
    place = lax.div(nest_offset[0], 3 * width)
    late = lax.rem(place, count) >= (count + 1) // 2
    return lax.switch(
        2 * (lax.div(place, count) - 1) + late.astype(jnp.int32),
        branches,
        nest_offset,
        nest_field,
        nest_area,
        parent_field,
        relax_rate,
        zonal_coef,
        merid_coef,
    )


def spots_of(mesh):
    line = list(mesh.devices[:, 0])
    found = []
    for index, device in enumerate(line):
        place = getattr(device, "coords", None)
        if place is None or len(place) != 3:
            return ()
        if place[1] != index // 2 % 2 or place[2] != index // 4:
            return ()
        found.append((place[1], place[2]))
    return tuple(found)


def solution(mesh):
    placed = (P(None, "band", "lon"), P("band", "lon"), P(None, "band", "lon"), P(), P(), P(), P())
    return jax.shard_map(
        functools.partial(on_device, spots_of(mesh)),
        mesh=mesh,
        in_specs=placed,
        out_specs=P(None, "band", "lon"),
        check_vma=False,
    )
```

```python
import functools

import jax
import jax.numpy as jnp
from jax import lax
from jax.experimental import pallas as pl
from jax.experimental.pallas import tpu as pltpu
from jax.sharding import PartitionSpec as P

NS = 3
HALO = NS
LANES = 128
HALF = LANES // 2
GROUP = 8
SMOOTH = 4
ORDER = ((0, 0), (1, 3), (2, 6))
MESH = pl.DeviceIdType.MESH
BULK, EAST, WEST, UP, DOWN, EDGES, DETOUR, ONWARD = range(8)


def routed(loads, here, there, amount):
    y, z = here
    while z != there[1]:
        step = 1 if there[1] > z else -1
        loads[y, z, step, 0] = loads.get((y, z, step, 0), 0) + amount
        z += step
    if y != there[0]:
        loads[y, z, 0, 1] = loads.get((y, z, 0, 1), 0) + amount


def detour(shift, forward, blocks, spots, part):
    total = len(spots)
    if not total or shift % total == 0:
        return 0, (), 0
    best = None
    for turn, choices in ((-2, ((), (3,), (2,), (2, 3))), (2, ((0,), (1,), (0, 1)))):
        for chosen in choices:
            for number in range(1, blocks) if chosen else (0,):
                loads = {}
                for here in range(total):
                    there = (here + shift) % total
                    share = number / blocks if here % 4 in chosen else 0
                    by = (here + turn) % total
                    if share and (spots[there][0] != spots[by][0] or there == by):
                        break
                    routed(loads, spots[here], spots[by], share)
                    routed(loads, spots[by], spots[there], share)
                    routed(loads, spots[here], spots[there], 1 - share)
                    beside = (here + (1 if forward else -1)) % total
                    routed(loads, spots[here], spots[beside], part)
                else:
                    key = (max(loads.values()) + (0.2 if number else 0.0), number)
                    if best is None or key < best[0]:
                        best = key, (turn, chosen, number)
    return best[1]


def chunk_width(par_cols):
    return max(w for w in range(1, HALF + 1) if par_cols % w == 0)


def rolled(x, by):
    by %= LANES
    return pltpu.roll(x, by, 1) if by else x


def kernel(
    shift, forward, split, width, way, off_ref, nest_hbm, area_hbm, parent_hbm, relax_hbm, zonal_hbm, merid_hbm,
    out_ref, nest, area, parent, relax, zonal, merid, select, spill, packed, got, east_out, east_got,
    west_out, west_got, edge_out, edge_got, hop, share, field, up_out, up_got, down_out, down_got,
    in_sems, send_sems, recv_sems,
):
    lon, band = lax.axis_index("lon"), lax.axis_index("band")
    lons, bands = lax.axis_size("lon"), lax.axis_size("band")
    levels, rows, cols = parent.shape
    lanes = field.shape[2]
    count = cols // width
    tail = lanes - cols
    blocks = levels // GROUP
    gone = list(range(split)) if forward else list(range(split, count))
    bulk = shift % lons != 0
    has_above, has_below = band > 0, band < bands - 1

    def at(ahead):
        return lax.rem(lon + ahead % lons, lons)

    barrier = pltpu.get_barrier_semaphore()

    def greet(x, y):
        pl.semaphore_signal(barrier, inc=1, device_id=(x, y), device_id_type=MESH)

    turn, chosen, detours = way
    partners = [1, -1] + ([shift, -shift] if bulk else [])
    if detours:
        partners += [turn, -turn, shift - turn, turn - shift]

        def among(index):
            found = lax.rem(index, 4) == chosen[0]
            for one in chosen[1:]:
                found = found | (lax.rem(index, 4) == one)
            return found

        leaves, helps = among(lon), among(at(-turn))
    for ahead in partners:
        greet(at(ahead), band)

    @pl.when(has_above)
    def _():
        greet(lon, band - 1)

    @pl.when(has_below)
    def _():
        greet(lon, band + 1)

    def load(index, source, target):
        return pltpu.make_async_copy(source, target, in_sems.at[index])

    def nest_load(block):
        part = pl.ds(block * GROUP, GROUP)
        return load(block, nest_hbm.at[part], nest.at[part])

    area_load = load(blocks, area_hbm, area)
    parent_load = load(blocks + 1, parent_hbm, parent)
    small = [
        load(blocks + 2 + k, source, target)
        for k, (source, target) in enumerate(
            [(relax_hbm, relax), (zonal_hbm, zonal), (merid_hbm, merid)]
        )
    ]
    area_load.start()
    for b in range(blocks):
        nest_load(b).start()
    parent_load.start()
    for one in small:
        one.start()

    unit = GROUP * count + 1
    last = blocks * unit
    kinds = [BULK, EAST, WEST, UP, DOWN, EDGES, DETOUR]
    lengths = [blocks + 1, blocks + 1, blocks + 1, blocks, blocks, 2, detours]
    firsts = {kind: sum(lengths[:i]) for i, kind in enumerate(kinds)}

    def copy(kind, index, source, target, x, y, at_target=None):
        first = firsts[kind if at_target is None else at_target]
        return pltpu.make_async_remote_copy(
            src_ref=source,
            dst_ref=target,
            send_sem=send_sems.at[kind],
            recv_sem=recv_sems.at[first + index],
            device_id=(x, y),
            device_id_type=MESH,
        )

    def bulk_copy(index, first, size):
        part = pl.ds(first, size)
        return copy(BULK, index, packed.at[part], got.at[part], at(shift), band)

    def detour_copy(index):
        part = pl.ds(index * unit, unit)
        return copy(DETOUR, index, packed.at[part], hop.at[part], at(turn), band)

    def onward_copy(index):
        part = pl.ds(index * unit, unit)
        return copy(
            ONWARD, index, hop.at[part], got.at[part], at(shift - turn), band, BULK
        )

    def east_copy(index, first, size):
        part = pl.ds(first, size)
        return copy(EAST, index, east_out.at[part], east_got.at[part], at(1), band)

    def west_copy(index, first, size):
        part = pl.ds(first, size)
        return copy(WEST, index, west_out.at[part], west_got.at[part], at(-1), band)

    def edge_copy(index):
        return copy(
            EDGES, index, edge_out.at[index], edge_got.at[index], at(1 if index else -1), band
        )

    def up_copy(index):
        return copy(UP, index, up_out.at[index], up_got.at[index], lon, band - 1)

    def down_copy(index):
        return copy(DOWN, index, down_out.at[index], down_got.at[index], lon, band + 1)

    arrived = got if bulk else packed
    offset = off_ref[0]
    start = lax.rem(lax.div(offset, 3), cols)
    within = lax.rem(start, width)
    lane = lax.broadcasted_iota(jnp.int32, (8, LANES), 1)
    low = lane < HALF
    spot = jnp.where(low, lane, lane - HALF)
    before = {c: spot < start - c * width for c in gone}
    here = {c: spot == start - c * width for c in gone}
    zero = jnp.zeros((8, LANES), jnp.float32)
    place = spot // 4
    is_right = spot < HALO
    is_left = (spot >= tail - HALO) & (spot < tail)

    def pack(values):
        tiles = []
        if width == HALF:
            for p in range(values.shape[1] // LANES):
                top = values[:8, p * LANES : (p + 1) * LANES]
                bottom = values[8:, p * LANES : (p + 1) * LANES]
                tiles.append(jnp.where(low, top, rolled(bottom, HALF)))
                tiles.append(jnp.where(low, rolled(top, HALF), bottom))
            return tiles
        pad = jnp.zeros((8, HALF - width), jnp.float32)
        for k in range(count + 1):
            part = values[:, k * width : (k + 1) * width]
            tiles.append(jnp.concatenate([part[:8], pad, part[8:], pad], axis=1))
        return tiles

    def unpack(tiles, end):
        if width == HALF and tail == HALF and count % 2:
            tiles = tiles + [end]
            top, bottom = [], []
            for x, y in zip(tiles[::2], tiles[1::2]):
                top.append(jnp.where(low, x, rolled(y, HALF)))
                bottom.append(jnp.where(low, rolled(x, HALF), y))
        else:
            top = [t[:, :width] for t in tiles] + [end[:, :tail]]
            bottom = [t[:, HALF : HALF + width] for t in tiles] + [end[:, HALF : HALF + tail]]
        return jnp.concatenate(
            [jnp.concatenate(top, axis=1), jnp.concatenate(bottom, axis=1)], axis=0
        )

    def first_part(tile, edge, k):
        rest = rolled(edge, -k)
        return {c: jnp.where(before[c], tile(c), jnp.where(here[c], rest, 0.0)) for c in gone}

    def second_part(tile):
        return {c: jnp.where(before[c], 0.0, tile(c)) for c in gone}

    def sent(tile, edge, k):
        return first_part(tile, edge, k) if forward else second_part(tile)

    def kept(tile, edge, k):
        parts = {c: tile(c) for c in range(count)}
        parts.update(second_part(tile) if forward else first_part(tile, edge, k))
        return parts

    def sums(values, planes, first):
        high = values.astype(jnp.bfloat16)
        rest = (values - high.astype(jnp.float32)).astype(jnp.bfloat16)
        by_column = jnp.dot(high, select[...], preferred_element_type=jnp.float32) + jnp.dot(
            rest, select[...], preferred_element_type=jnp.float32
        )
        edge = zero
        for k in range(planes):
            tiles = pack(by_column[k * rows : (k + 1) * rows])
            for c in range(count):
                packed[first + k * count + c] = tiles[c]
            edge = edge + rolled(tiles[count], k)
        packed[first + planes * count] = edge

    spread = select.shape[1]
    slot_of = lax.broadcasted_iota(jnp.int32, (8, spread), 1)
    column = jnp.where(slot_of >= start, slot_of - start, slot_of - start + cols)
    column = jnp.where(
        slot_of < cols, column, jnp.where(slot_of == cols + within, cols, -HALF)
    )
    lowest = (column * 3 - lax.rem(offset, 3))[:1]
    strip = max(n for n in range(16, 65, 16) if select.shape[0] % n == 0)
    ramp = lax.broadcasted_iota(jnp.int32, (strip, spread), 0) - lowest

    def choose(step, carry):
        cell = ramp + step * strip
        hit = (cell >= 0) & (cell < 3)
        select[pl.ds(pl.multiple_of(step * strip, strip), strip), :] = jnp.where(
            hit, 1.0, 0.0
        ).astype(jnp.bfloat16)
        return carry

    lax.fori_loop(0, select.shape[0] // strip, choose, 0)

    cells = area.shape[1]

    def by_rows(planes):
        height = planes[0].shape[0]
        for t in range(spill.shape[0]):
            edge = min(cells, (t + 1) * LANES)
            for k, plane in enumerate(planes):
                spill[t, k * height : (k + 1) * height, : edge - t * LANES] = plane[:, t * LANES : edge]
        third = len(planes) * rows
        tiles = []
        for t in range(spill.shape[0]):
            edge = min(cells, (t + 1) * LANES)
            tile = (
                spill.at[t][pl.ds(0, third, stride=3), :]
                + spill.at[t][pl.ds(1, third, stride=3), :]
                + spill.at[t][pl.ds(2, third, stride=3), :]
            )
            tiles.append(tile[:, : edge - t * LANES])
        return jnp.concatenate(tiles, axis=1)

    area_load.wait()
    sums(by_rows([area[...]]), 1, last)
    pl.semaphore_wait(
        barrier, len(partners) + has_above.astype(jnp.int32) + has_below.astype(jnp.int32)
    )
    if bulk:
        bulk_copy(blocks, last, count + 1).start()

    def front(block, carry):
        nest_load(block).wait()
        weight = area[...]
        planes = [nest[block * GROUP + k] * weight for k in range(GROUP)]
        sums(by_rows(planes), GROUP, block * unit)
        if detours:
            around = leaves & (block < detours)

            @pl.when(around)
            def _():
                detour_copy(block).start()

            @pl.when(jnp.logical_not(around))
            def _():
                bulk_copy(block, block * unit, unit).start()
        elif bulk:
            bulk_copy(block, block * unit, unit).start()
        return carry

    lax.fori_loop(0, blocks, front, 0)

    parent_load.wait()
    blank = jnp.zeros((rows, tail), jnp.float32)
    head = (cols - HALO) // LANES * LANES

    def edges(block, carry):
        first, final = zero, zero
        for k in range(GROUP):
            wide = jnp.concatenate([parent[block * GROUP + k], blank], axis=1)
            for half, part in enumerate([wide[:8], wide[8:]]):
                mine = (place == k) & (low if half == 0 else ~low)
                to = 4 * k + HALF * half
                first = jnp.where(mine, rolled(part[:, :LANES], to), first)
                end = part[:, head : head + LANES]
                final = jnp.where(mine, rolled(end, to - (cols - HALO - head)), final)
        edge_out[0, block] = first
        edge_out[1, block] = final
        return carry

    lax.fori_loop(0, blocks, edges, 0)
    for side in range(2):
        edge_copy(side).start()

    @pl.when(jnp.logical_not(has_above))
    def _():
        down_got[...] = jnp.zeros_like(down_got)

    @pl.when(jnp.logical_not(has_below))
    def _():
        up_got[...] = jnp.zeros_like(up_got)

    def tile_of(first):
        return lambda c: arrived[first + c]

    main = len(gone)

    def sizes(planes):
        return (planes * main + 1, 1) if forward else (1, planes * main + 1)

    def hand_on(first, planes, index, target):
        edge = arrived[first + planes * count]
        east_pack, west_pack = zero, zero
        for k in range(planes):
            tile = tile_of(first + k * count)
            out = sent(tile, edge, k)
            keep = kept(tile, edge, k)
            main_out = east_out if forward else west_out
            for j, c in enumerate(gone):
                main_out[target[0 if forward else 1] + k * main + j] = out[c]
            mine = place == k
            east_pack = jnp.where(
                mine, rolled(keep[count - 1], 4 * k - (width - HALO)), east_pack
            )
            west_pack = jnp.where(mine, rolled(keep[0], 4 * k), west_pack)
        east_size, west_size = sizes(planes)
        east_out[target[0] + east_size - 1] = east_pack
        west_out[target[1] + west_size - 1] = west_pack
        east_copy(index, target[0], east_size).start()
        west_copy(index, target[1], west_size).start()

    def assembled(first, planes, k, target, fill):
        edge = arrived[first + planes * count]
        tile = tile_of(first + k * count)
        out = sent(tile, edge, k)
        parts = kept(tile, edge, k)
        east_size, west_size = sizes(planes)
        main_got = east_got if forward else west_got
        for j, c in enumerate(gone):
            value = main_got[target[0 if forward else 1] + k * main + j]
            parts[c] = parts[c] + value
        left = rolled(east_got[target[0] + east_size - 1], tail - HALO - 4 * k)
        right = rolled(west_got[target[1] + west_size - 1], -4 * k)
        if forward:
            right = right + out[0]
        else:
            left = left + rolled(out[count - 1], tail - width)
        end = jnp.where(is_right, right, jnp.where(is_left, left, fill))
        return unpack([parts[c] for c in range(count)], end)

    def targets(block):
        east_size, west_size = sizes(GROUP)
        return block * east_size, block * west_size

    def wait_sides(index, planes, target):
        east_size, west_size = sizes(planes)
        east_copy(index, target[0], east_size).wait_recv()
        west_copy(index, target[1], west_size).wait_recv()

    if bulk:
        bulk_copy(blocks, last, count + 1).wait_recv()
    hand_on(last, 1, blocks, targets(blocks))

    def place_of(due):
        return lax.rem(due + detours, blocks) if detours else due

    def take(due):
        block = place_of(due)
        if detours:

            @pl.when(helps & (due < detours))
            def _():
                detour_copy(due).wait_recv()
                onward_copy(due).start()

        if bulk:
            bulk_copy(block, block * unit, unit).wait_recv()
        hand_on(block * unit, GROUP, block, targets(block))

    def blend(due):
        block = place_of(due)

        @pl.when(due == 0)
        def _():
            wait_sides(blocks, 1, targets(blocks))
            share[...] = 1.0 / assembled(last, 1, 0, targets(blocks), 1.0)
            for one in small:
                one.wait()
            for side in range(2):
                edge_copy(side).wait_recv()

        wait_sides(block, GROUP, targets(block))
        from_east, from_west = edge_got[0, block], edge_got[1, block]
        for k in range(GROUP):
            level = block * GROUP + k
            ratio = assembled(block * unit, GROUP, k, targets(block), 0.0) * share[...]
            end = jnp.where(
                is_right,
                rolled(from_east, -4 * k),
                jnp.where(is_left, rolled(from_west, tail - HALO - 4 * k), 0.0),
            )
            ends = jnp.concatenate([end[:, :tail], end[:, HALF : HALF + tail]], axis=0)
            before_it = jnp.concatenate([parent[level], ends], axis=1)
            value = before_it + relax[level] * (ratio - before_it)
            field[level] = value
            for j in range(HALO):
                up_out[block, j, k : k + 1, :] = value[j : j + 1]
                down_out[block, j, k : k + 1, :] = value[rows - HALO + j : rows - HALO + j + 1]

        @pl.when(has_above)
        def _():
            up_copy(block).start()

        @pl.when(has_below)
        def _():
            down_copy(block).start()

    tall = rows + 8
    row = lax.broadcasted_iota(jnp.int32, (tall, lanes), 0)
    valid = (
        (row < rows)
        | ((row < rows + HALO) & has_below)
        | ((row >= tall - HALO) & has_above)
    )
    spare = jnp.zeros((8 - 2 * HALO, lanes), jnp.float32)

    def smooth(due):
        block = place_of(due)

        @pl.when(has_above)
        def _():
            down_copy(block).wait_recv()

        @pl.when(has_below)
        def _():
            up_copy(block).wait_recv()

        def some(step, carry):
            group = [step * SMOOTH + g for g in range(SMOOTH)]
            values = []
            for k in group:
                extra = [up_got[block, j, pl.ds(k, 1), :] for j in range(HALO)] + [spare]
                extra += [down_got[block, j, pl.ds(k, 1), :] for j in range(HALO)]
                values.append(jnp.concatenate([field[block * GROUP + k]] + extra, axis=0))
            zonals = [zonal[block * GROUP + k] for k in group]
            merids = [merid[block * GROUP + k] for k in group]
            for sweep in range(NS):
                sides = [pltpu.roll(v, 1, 1) + pltpu.roll(v, lanes - 1, 1) for v in values]
                values = [v + z * (s - 2.0 * v) for v, z, s in zip(values, zonals, sides)]
                sides = [pltpu.roll(v, 1, 0) + pltpu.roll(v, tall - 1, 0) for v in values]
                values = [
                    jnp.where(valid, v + m * (s - 2.0 * v), 0.0)
                    for v, m, s in zip(values, merids, sides)
                ]
            for k, value in zip(group, values):
                out_ref[block * GROUP + k] = value[:rows, :cols]
            return carry

        lax.fori_loop(0, GROUP // SMOOTH, some, 0)

    def advance(step, carry):
        for stage, lag in ORDER:
            due = step - lag

            @pl.when((due >= 0) & (due < blocks))
            def _():
                [take, blend, smooth][stage](due)

        return carry

    lax.fori_loop(0, blocks + max(lag for _, lag in ORDER), advance, 0)

    def sent_all(kind, source, target):
        copy(kind, 0, source, target, lon, band).wait_send()

    if detours:
        early = pl.ds(0, detours * unit)
        later = pl.ds(detours * unit, packed.shape[0] - detours * unit)

        @pl.when(leaves)
        def _():
            sent_all(DETOUR, packed.at[early], hop)
            sent_all(BULK, packed.at[later], got.at[later])

        @pl.when(jnp.logical_not(leaves))
        def _():
            sent_all(BULK, packed, got)

        @pl.when(helps)
        def _():
            copy(ONWARD, 0, hop, got.at[early], lon, band, BULK).wait_send()
    elif bulk:
        sent_all(BULK, packed, got)
    sent_all(EAST, east_out, east_got)
    sent_all(WEST, west_out, west_got)
    sent_all(EDGES, edge_out, edge_got)

    @pl.when(has_above)
    def _():
        sent_all(UP, up_out, up_got)

    @pl.when(has_below)
    def _():
        sent_all(DOWN, down_out, down_got)


def fused(
    shift, forward, split, width, spots, number, offset, nest, area, parent, relax, zonal, merid
):
    levels, rows, cols = parent.shape
    cells = nest.shape[2]
    count = cols // width
    lanes = (cols + 2 * HALO + LANES - 1) // LANES * LANES
    spread = ((count + 1) * width + LANES - 1) // LANES * LANES
    blocks = levels // GROUP
    assert count > 1 and rows == 16 and levels % GROUP == 0 and 4 * GROUP <= HALF
    main = split if forward else count - split
    way = detour(shift, forward, blocks, spots, main / count)
    unit = GROUP * count + 1
    many, few = blocks * (GROUP * main + 1) + main + 1, blocks + 1
    east_tiles, west_tiles = (many, few) if forward else (few, many)
    moved = blocks * (GROUP * count + 1) + count + 1

    def tiles(*shape):
        return pltpu.VMEM(shape + (8, LANES), jnp.float32)

    strip = pltpu.VMEM((blocks, HALO, GROUP, lanes), jnp.float32)
    hbm = pl.BlockSpec(memory_space=pl.ANY)
    scalars = pltpu.SMEM((levels,), jnp.float32)
    return pl.pallas_call(
        functools.partial(kernel, shift, forward, split, width, way),
        out_shape=jax.ShapeDtypeStruct(parent.shape, jnp.float32),
        in_specs=[pl.BlockSpec(memory_space=pltpu.SMEM)] + [hbm] * 6,
        out_specs=pl.BlockSpec(memory_space=pltpu.VMEM),
        scratch_shapes=[
            pltpu.VMEM(nest.shape, jnp.float32),
            pltpu.VMEM(area.shape, jnp.float32),
            pltpu.VMEM(parent.shape, jnp.float32),
            scalars,
            scalars,
            scalars,
            pltpu.VMEM((cells, spread), jnp.bfloat16),
            pltpu.VMEM(((cells + LANES - 1) // LANES, GROUP * nest.shape[1], LANES), jnp.float32),
            tiles(moved),
            tiles(moved),
            tiles(east_tiles),
            tiles(east_tiles),
            tiles(west_tiles),
            tiles(west_tiles),
            tiles(2, blocks),
            tiles(2, blocks),
            tiles(max(way[2], 1) * unit),
            pltpu.VMEM((rows, lanes), jnp.float32),
            pltpu.VMEM((levels, rows, lanes), jnp.float32),
            strip,
            strip,
            strip,
            strip,
            pltpu.SemaphoreType.DMA((blocks + 5,)),
            pltpu.SemaphoreType.DMA((8 if way[2] else 6,)),
            pltpu.SemaphoreType.DMA((5 * blocks + 5 + way[2],)),
        ],
        compiler_params=pltpu.CompilerParams(
            collective_id=number, has_side_effects=True, vmem_limit_bytes=24 << 20
        ),
    )(offset, nest, area, parent, relax, zonal, merid)


def on_device(spots, nest_field, nest_area, parent_field, nest_offset, relax_rate, zonal_coef, merid_coef):
    cols = parent_field.shape[2]
    width = chunk_width(cols)
    count = cols // width
    lons = lax.axis_size("lon")
    wide, narrow = (count + 1) // 2, count // 2
    branches = []
    for steps in range(1, lons):
        split = wide if steps <= lons // 2 else narrow
        for forward in (True, False):
            shift = steps if forward else steps + 1
            branches.append(
                functools.partial(fused, shift, forward, split, width, spots, len(branches))
            )
    place = lax.div(nest_offset[0], 3 * width)
    steps = lax.div(place, count)
    late = lax.rem(place, count) >= jnp.where(steps <= lons // 2, wide, narrow)
    return lax.switch(
        2 * (steps - 1) + late.astype(jnp.int32),
        branches,
        nest_offset,
        nest_field,
        nest_area,
        parent_field,
        relax_rate,
        zonal_coef,
        merid_coef,
    )


def spots_of(mesh):
    line = list(mesh.devices[:, 0])
    found = []
    for index, device in enumerate(line):
        place = getattr(device, "coords", None)
        if place is None or len(place) != 3:
            return ()
        if place[1] != index // 2 % 2 or place[2] != index // 4:
            return ()
        found.append((place[1], place[2]))
    return tuple(found)


def solution(mesh):
    placed = (P(None, "band", "lon"), P("band", "lon"), P(None, "band", "lon"), P(), P(), P(), P())
    return jax.shard_map(
        functools.partial(on_device, spots_of(mesh)),
        mesh=mesh,
        in_specs=placed,
        out_specs=P(None, "band", "lon"),
        check_vma=False,
    )
```
